32 devices in a mesh: row: 8 (over z, y), col: 4 (over x, core).
Axes of the slice: x: 2, y: 2, z: 4, core: 2. Of those that a mesh axis runs over, the one named last changes fastest.
Arguments:
- image_embed: float32 [4096, 1152], P(('row', 'col')), may hold values from -150 to 150, as said below
- text_embed: float32 [4096, 1152], P(('row', 'col')), may hold values from -150 to 150
- log_scale: float32 [1], replicated, may hold values from 1.8 to 2.6
- bias: float32 [1], replicated, may hold values from -6 to -3
Outputs:
- loss: float32 [1], replicated
- image_grad: float32 [4096, 1152], P(('row', 'col'))
- text_grad: float32 [4096, 1152], P(('row', 'col'))
The draws below stay inside these ranges and needn't reach their ends.
Inputs may be any that keep to these rules, and one draw needn't show every extreme that they name: Row i of image_embed and row i of text_embed are correlated.
All inputs are finite; a program needn't handle non-finite values.
Results may differ from the reference program's by a relative error of at most 0.0046.
Values may be sent and summed in bfloat16 or wider, within the bound.
No kernel may reach another device: no remote copies, remote signals or barrier semaphores. Data moves between devices by JAX's collectives and lax.ppermute only.
A program may use at most 64 MiB of HBM per device.

```python
import math
import jax
import jax.numpy as jnp
from jax import lax

D = 1152
GROUP = 512
TOTAL = 4096
N_ROW = 8


def pair_draw(key):
    keys = jax.random.split(jax.random.fold_in(key, 7), 6)
    base = jnp.clip(jax.random.normal(keys[0], (TOTAL, D), jnp.float32), -4.0, 4.0)
    noise_img = jnp.clip(jax.random.normal(keys[1], (TOTAL, D), jnp.float32), -4.0, 4.0)
    noise_txt = jnp.clip(jax.random.normal(keys[2], (TOTAL, D), jnp.float32), -4.0, 4.0)
    column = jnp.exp(jax.random.uniform(keys[3], (1, D), jnp.float32, 0.0, math.log(10.0)))
    row_img = jnp.exp(jax.random.uniform(keys[4], (TOTAL, 1), jnp.float32, 0.0, math.log(10.0)))
    row_txt = jnp.exp(jax.random.uniform(keys[5], (TOTAL, 1), jnp.float32, 0.0, math.log(10.0)))
    divisor = jnp.sqrt(jnp.float32(D))
    image = (base + 0.8 * noise_img) * column * row_img / divisor
    text = (0.7 * base + noise_txt) * column * row_txt / divisor
    return (image, text)


def draw_image_embed(key, part):
    return pair_draw(key)[0]


def draw_text_embed(key, part):
    return pair_draw(key)[1]


def setup_inputs(seed: int = 0) -> dict:
    splits = jax.random.split(jax.random.key(seed), 5)
    return {
        "image_embed": draw_image_embed(jax.random.fold_in(splits[4], 71), 0),
        "text_embed": draw_text_embed(jax.random.fold_in(splits[4], 71), 0),
        "log_scale": jnp.clip(jax.random.uniform(splits[2], (1,), jnp.float32, 1.8, 2.6), 1.8, 2.6),
        "bias": jnp.clip(jax.random.uniform(splits[3], (1,), jnp.float32, -6.0, -3.0), -6.0, -3.0),
    }


def unit_rows(values):
    inverse = 1.0 / jnp.sqrt(lax.optimization_barrier(jnp.sum(values * values, axis=1, keepdims=True)) + 1e-06)
    return (values * inverse, inverse)

def back_rows(grad_unit, unit, inverse):
    return inverse * (grad_unit - lax.optimization_barrier(jnp.sum(grad_unit * unit, axis=1, keepdims=True)) * unit)

def reference(image_embed, text_embed, log_scale, bias):
    scale = jnp.exp(log_scale[0])
    offset = bias[0]

    def one_batch(pair):
        images, texts = pair
        img_unit, img_inv = unit_rows(images)
        txt_unit, txt_inv = unit_rows(texts)
        img_b = img_unit.astype(jnp.bfloat16)
        txt_b = txt_unit.astype(jnp.bfloat16)
        logits = scale * jnp.dot(img_b, txt_b.T, preferred_element_type=jnp.float32) + offset
        index = jnp.arange(GROUP, dtype=jnp.int32)
        sign = jnp.where(index[:, None] == index[None, :], 1.0, -1.0).astype(logits.dtype)
        total = jnp.sum(jax.nn.softplus(-sign * logits))
        weight = (-sign * jax.nn.sigmoid(-sign * logits)).astype(jnp.bfloat16)
        img_gu = scale * jnp.dot(weight, txt_b, preferred_element_type=jnp.float32)
        txt_gu = scale * jnp.dot(weight.T, img_b, preferred_element_type=jnp.float32)
        return (total, back_rows(img_gu, img_unit, img_inv), back_rows(txt_gu, txt_unit, txt_inv))
    images = image_embed.reshape(N_ROW, GROUP, D)
    texts = text_embed.reshape(N_ROW, GROUP, D)
    totals, image_grad, text_grad = lax.map(one_batch, (images, texts))
    loss = (jnp.sum(totals) / TOTAL).reshape(1)
    return (loss, image_grad.reshape(TOTAL, D), text_grad.reshape(TOTAL, D))
```

```python
import jax
import jax.numpy as jnp
from jax import lax
from jax.sharding import PartitionSpec as P


def moved(value, axis, target):
    count = lax.axis_size(axis)
    return lax.ppermute(value, axis, [(i, target(i)) for i in range(count)])


def unit_rows(values):
    inverse = 1.0 / jnp.sqrt(jnp.sum(values * values, axis=1, keepdims=True) + 1e-06)
    return (values * inverse, inverse)


def back_rows(grad_unit, unit, inverse):
    return inverse * (grad_unit - jnp.sum(grad_unit * unit, axis=1, keepdims=True) * unit)


def dot_t(a, b):
    return lax.dot_general(a, b, (((1,), (1,)), ((), ())), preferred_element_type=jnp.float32)


def dot_n(a, b):
    return jnp.dot(a, b, preferred_element_type=jnp.float32)


def over_axis(value, axis):
    count = lax.axis_size(axis)
    if count & (count - 1):
        return lax.psum(value, axis)
    step = 1
    while step < count:
        value = value + moved(value, axis, lambda i: i ^ step)
        step *= 2
    return value


def gathered(mine, cores):
    count = lax.axis_size("col")
    chips = count // cores
    blocks = [mine]
    for hop in range(1, chips):
        blocks.append(moved(mine, "col", lambda i: (i + hop * cores) % count))
    others = []
    for core in range(1, cores):
        for block in blocks:
            others.append(moved(block, "col", lambda i: i // cores * cores + (i + core) % cores))
    return blocks + others


def local(image_embed, text_embed, log_scale, bias):
    rows = image_embed.shape[0]
    n_row = lax.axis_size("row")
    n_col = lax.axis_size("col")
    cores = 2 if n_col % 2 == 0 else 1
    scale = jnp.exp(log_scale[0])
    offset = bias[0]
    txt_unit, txt_inv = unit_rows(text_embed)
    txt_b = txt_unit.astype(jnp.bfloat16)
    img_unit, img_inv = unit_rows(image_embed)
    img_b = img_unit.astype(jnp.bfloat16)
    texts = gathered(txt_b, cores)
    images = gathered(img_b, cores)
    eye = lax.broadcasted_iota(jnp.int32, (rows, rows), 0) == lax.broadcasted_iota(jnp.int32, (rows, rows), 1)
    plus = jnp.where(eye, 1.0, -1.0).astype(jnp.float32)
    minus = jnp.full((rows, rows), -1.0, jnp.float32)

    loss_sum = jnp.zeros((), jnp.float32)
    img_sum = None
    for j, slab in enumerate(texts):
        sign = plus if j == 0 else minus
        logits = scale * dot_t(img_b, slab) + offset
        loss_sum = loss_sum + jnp.sum(jax.nn.softplus(-sign * logits))
        weight = (-sign * jax.nn.sigmoid(-sign * logits)).astype(jnp.bfloat16)
        term = dot_n(weight, slab)
        img_sum = term if img_sum is None else img_sum + term
    txt_sum = None
    for j, slab in enumerate(images):
        sign = plus if j == 0 else minus
        logits = scale * dot_t(txt_b, slab) + offset
        weight = (-sign * jax.nn.sigmoid(-sign * logits)).astype(jnp.bfloat16)
        term = dot_n(weight, slab)
        txt_sum = term if txt_sum is None else txt_sum + term
    total = jnp.broadcast_to(loss_sum, (1, 128))
    total = over_axis(over_axis(total, "row"), "col")
    loss = total[0, :1] / (rows * n_row * n_col)
    image_grad = back_rows(scale * img_sum, img_unit, img_inv)
    text_grad = back_rows(scale * txt_sum, txt_unit, txt_inv)
    return (loss, image_grad, text_grad)


def solution(mesh):
    in_specs = (P(("row", "col"), None), P(("row", "col"), None), P(), P())
    out_specs = (P(), P(("row", "col"), None), P(("row", "col"), None))
    return jax.shard_map(local, mesh=mesh, in_specs=in_specs, out_specs=out_specs, check_vma=False)
```

```python
import functools

import jax
import jax.numpy as jnp
from jax import lax
from jax.experimental import pallas as pl
from jax.experimental.pallas import tpu as pltpu
from jax.sharding import PartitionSpec as P


GRANT = 12 << 20
LANES = 128
VMEM = pl.BlockSpec(memory_space=pltpu.VMEM)
HBM = pl.BlockSpec(memory_space=pltpu.HBM)


def moved(value, axis, target):
    count = lax.axis_size(axis)
    return lax.ppermute(value, axis, [(i, target(i)) for i in range(count)])


def kernel_call(body, outs, ins, scratch=(), in_hbm=0, out_hbm=False, flops=0):
    return pl.pallas_call(
        body,
        out_shape=outs,
        in_specs=[HBM] * in_hbm + [VMEM] * (len(ins) - in_hbm),
        out_specs=jax.tree.map(lambda _: HBM if out_hbm else VMEM, outs),
        scratch_shapes=list(scratch),
        compiler_params=pltpu.CompilerParams(vmem_limit_bytes=GRANT),
        cost_estimate=pl.CostEstimate(flops=flops, bytes_accessed=0, transcendentals=0),
    )(*ins)


def dot_t(a, b):
    return lax.dot_general(a, b, (((1,), (1,)), ((), ())), preferred_element_type=jnp.float32)


def dot_n(a, b):
    return jnp.dot(a, b, preferred_element_type=jnp.float32)


def eye_signs(rows):
    eye = lax.broadcasted_iota(jnp.int32, (rows, rows), 0) == lax.broadcasted_iota(jnp.int32, (rows, rows), 1)
    return jnp.where(eye, 1.0, -1.0).astype(jnp.float32)


def softplus(v):
    return jnp.maximum(v, 0.0) + jnp.log1p(jnp.exp(-jnp.abs(v)))


def weights(arg, sign):
    return (-sign / (1.0 + jnp.exp(-arg))).astype(jnp.bfloat16)


def logits_of(par_ref, a, b):
    return par_ref[0:1, 0:1] * dot_t(a, b) + par_ref[1:2, 0:1]


def unit_parts(values):
    inverse = 1.0 / jnp.sqrt(jnp.sum(values * values, axis=1, keepdims=True) + 1e-06)
    return values * inverse, inverse


def image_norm_kernel(raw_ref, b_ref, unit_ref, inv_ref):
    unit, inverse = unit_parts(raw_ref[...])
    b_ref[...] = unit.astype(jnp.bfloat16)
    unit_ref[...] = unit
    inv_ref[...] = jnp.broadcast_to(inverse, inv_ref.shape)


def text_parts_kernel(raw_ref, unit_ref, inv_ref):
    unit, inverse = unit_parts(raw_ref[...])
    unit_ref[...] = unit
    inv_ref[...] = jnp.broadcast_to(inverse, inv_ref.shape)


def near_kernel(count, par_ref, txt_ref, img_ref, *refs):
    texts = (txt_ref,) + refs[: count - 1]
    images = (img_ref,) + refs[count - 1 : 2 * count - 2]
    img_sum_ref, txt_sum_ref, loss_ref = refs[2 * count - 2 :]
    rows = txt_ref.shape[0]
    img_sum = txt_sum = loss = None
    for j in range(count):
        sign = eye_signs(rows) if j == 0 else -1.0
        arg = -sign * logits_of(par_ref, img_ref[...], texts[j][...])
        term = dot_n(weights(arg, sign), texts[j][...])
        img_sum = term if j == 0 else img_sum + term
        arg = -sign * logits_of(par_ref, txt_ref[...], images[j][...])
        term = dot_n(weights(arg, sign), images[j][...])
        txt_sum = term if j == 0 else txt_sum + term
        part = jnp.sum(softplus(arg), axis=0, keepdims=True)
        loss = part if j == 0 else loss + part
    img_sum_ref[...] = img_sum
    txt_sum_ref[...] = txt_sum
    loss_ref[...] = jnp.broadcast_to(jnp.sum(loss, axis=1, keepdims=True), loss_ref.shape)


def far_loss_kernel(n_img, par_ref, near_ref, *refs):
    images, texts, loss_ref = refs[:n_img], refs[n_img:-1], refs[-1]
    loss = None
    for image in images:
        for text in texts:
            part = jnp.sum(softplus(logits_of(par_ref, image[...], text[...])), axis=0, keepdims=True)
            loss = part if loss is None else loss + part
    loss_ref[...] = near_ref[...] + jnp.broadcast_to(jnp.sum(loss, axis=1, keepdims=True), loss_ref.shape)


def sum_kernel(par_ref, own_ref, carry_ref, *refs):
    total = carry_ref[...]
    for block in refs[:-1]:
        arg = logits_of(par_ref, own_ref[...], block[...])
        total = total + dot_n(weights(arg, -1.0), block[...])
    refs[-1][...] = total


def far_sum(params, own, carry, blocks):
    rows, width = own.shape
    return kernel_call(
        sum_kernel,
        jax.ShapeDtypeStruct((rows, width), jnp.float32),
        (params, own, carry, *blocks),
        flops=4 * rows * rows * width * len(blocks),
    )


def last_kernel(count, par_ref, own_ref, carry_ref, unit_ref, inv_ref, *refs):
    blocks, (out_ref, buf, sems) = refs[:count], refs[count:]
    parts = sems.shape[0]
    step = buf.shape[0] // parts
    scale = par_ref[0:1, 0:1]
    gates = [weights(logits_of(par_ref, own_ref[...], block[...]), -1.0) for block in blocks]
    copies = []
    for k in range(parts):
        at = pl.ds(k * step, step)
        total = carry_ref[at, :]
        for gate, block in zip(gates, blocks):
            total = total + dot_n(gate[k * step : (k + 1) * step, :], block[...])
        grad = scale * total
        unit = unit_ref[at, :]
        inverse = inv_ref[at, 0:1]
        buf[at, :] = inverse * (grad - jnp.sum(grad * unit, axis=1, keepdims=True) * unit)
        copy = pltpu.make_async_copy(buf.at[at], out_ref.at[at], sems.at[k])
        copy.start()
        copies.append(copy)
    for copy in copies:
        copy.wait()


def finished(params, own, carry, unit, inverse, blocks):
    rows, width = own.shape
    return kernel_call(
        functools.partial(last_kernel, len(blocks)),
        jax.ShapeDtypeStruct((rows, width), jnp.float32),
        (params, own, carry, unit, inverse, *blocks),
        [pltpu.VMEM((rows, width), jnp.float32), pltpu.SemaphoreType.DMA((4,))],
        out_hbm=True,
        flops=4 * rows * rows * width * len(blocks),
    )


def summed(value):
    hops = []
    for axis in ("col", "row", "col"):
        count = lax.axis_size(axis)
        if count & (count - 1):
            return lax.psum(value, ("row", "col"))
        steps = [1 << k for k in range(count.bit_length() - 1)]
        if axis == "col":
            steps = steps[1:] if hops else steps[:1]
        hops += [(axis, step) for step in steps]
    for axis, step in hops:
        value = value + moved(value, axis, lambda i: i ^ step)
    return value


def across(mine, cores):
    count = lax.axis_size("col")
    return [moved(mine, "col", lambda i: (i + hop * cores) % count) for hop in range(1, count // cores)]


def partners(block, cores):
    return [moved(block, "col", lambda i: i // cores * cores + (i + core) % cores) for core in range(1, cores)]


def step(image_embed, text_embed, log_scale, bias):
    rows, width = image_embed.shape
    n_row = lax.axis_size("row")
    n_col = lax.axis_size("col")
    cores = 2 if n_col % 2 == 0 else 1
    params = jnp.broadcast_to(jnp.stack([jnp.exp(log_scale), bias]), (2, LANES))
    f32 = jnp.float32
    flops = 2 * rows * rows * width

    wide = jax.ShapeDtypeStruct((rows, width), f32)
    column = jax.ShapeDtypeStruct((rows, LANES), f32)
    txt_b = unit_parts(text_embed)[0].astype(jnp.bfloat16)
    txt_far = across(txt_b, cores)
    half = jax.ShapeDtypeStruct((rows, width), jnp.bfloat16)
    img_b, img_unit, img_inv = kernel_call(image_norm_kernel, (half, wide, column), (image_embed,))
    txt_unit, txt_inv = kernel_call(text_parts_kernel, (wide, column), (text_embed,))
    img_far = across(img_b, cores)
    txt_near = partners(txt_b, cores)
    img_near = partners(img_b, cores)
    terms = jax.ShapeDtypeStruct((1, LANES), f32)
    img_sum, txt_sum, loss = kernel_call(
        functools.partial(near_kernel, cores),
        (wide, wide, terms),
        (params, txt_b, img_b, *txt_near, *img_near),
        flops=4 * flops * cores,
    )
    if txt_far:
        txt_rest = [other for block in txt_far for other in partners(block, cores)]
        loss = kernel_call(
            functools.partial(far_loss_kernel, cores),
            terms,
            (params, loss, img_b, *img_near, *txt_far),
            flops=flops * cores * len(txt_far),
        )
        img_rest = [other for block in img_far for other in partners(block, cores)]
        txt_sum = far_sum(params, txt_b, txt_sum, img_far)
    image_grad = finished(params, img_b, img_sum, img_unit, img_inv, txt_far + txt_rest)
    text_grad = finished(params, txt_b, txt_sum, txt_unit, txt_inv, img_rest)
    total = summed(loss)
    loss = total[0, :1] / (rows * n_row * n_col)
    return (loss, image_grad, text_grad)


def solution(mesh):
    in_specs = (P(("row", "col"), None), P(("row", "col"), None), P(), P())
    out_specs = (P(), P(("row", "col"), None), P(("row", "col"), None))
    return jax.shard_map(step, mesh=mesh, in_specs=in_specs, out_specs=out_specs, check_vma=False)
```

```python
import functools

import jax
import jax.numpy as jnp
from jax import lax
from jax.experimental import pallas as pl
from jax.experimental.pallas import tpu as pltpu
from jax.sharding import PartitionSpec as P


GRANT = 12 << 20
LANES = 128
VMEM = pl.BlockSpec(memory_space=pltpu.VMEM)
HBM = pl.BlockSpec(memory_space=pltpu.HBM)


def moved(value, axis, target):
    count = lax.psum(1, axis)
    return lax.ppermute(value, axis, [(i, target(i)) for i in range(count)])


def kernel_call(body, outs, ins, scratch=(), in_hbm=0, out_hbm=False, flops=0):
    return pl.pallas_call(
        body,
        out_shape=outs,
        in_specs=[HBM] * in_hbm + [VMEM] * (len(ins) - in_hbm),
        out_specs=jax.tree.map(lambda _: HBM if out_hbm else VMEM, outs),
        scratch_shapes=list(scratch),
        compiler_params=pltpu.CompilerParams(vmem_limit_bytes=GRANT),
        cost_estimate=pl.CostEstimate(flops=flops, bytes_accessed=0, transcendentals=0),
    )(*ins)


def dot_t(a, b):
    return lax.dot_general(a, b, (((1,), (1,)), ((), ())), preferred_element_type=jnp.float32)


def dot_n(a, b):
    return jnp.dot(a, b, preferred_element_type=jnp.float32)


def eye_signs(rows):
    eye = lax.broadcasted_iota(jnp.int32, (rows, rows), 0) == lax.broadcasted_iota(jnp.int32, (rows, rows), 1)
    return jnp.where(eye, 1.0, -1.0).astype(jnp.float32)


def softplus(v):
    return jnp.maximum(v, 0.0) + jnp.log1p(jnp.exp(-jnp.abs(v)))


def weights(arg, sign):
    return (-sign / (1.0 + jnp.exp(-arg))).astype(jnp.bfloat16)


def logits_of(par_ref, a, b):
    return par_ref[0:1, 0:1] * dot_t(a, b) + par_ref[1:2, 0:1]


def unit_parts(values):
    inverse = 1.0 / jnp.sqrt(jnp.sum(values * values, axis=1, keepdims=True) + 1e-06)
    return values * inverse, inverse


def image_norm_kernel(raw_ref, b_ref, unit_ref, inv_ref):
    unit, inverse = unit_parts(raw_ref[...])
    b_ref[...] = unit.astype(jnp.bfloat16)
    unit_ref[...] = unit
    inv_ref[...] = jnp.broadcast_to(inverse, inv_ref.shape)


def text_parts_kernel(raw_ref, unit_ref, inv_ref):
    unit, inverse = unit_parts(raw_ref[...])
    unit_ref[...] = unit
    inv_ref[...] = jnp.broadcast_to(inverse, inv_ref.shape)


def near_kernel(count, par_ref, txt_ref, img_ref, *refs):
    texts = (txt_ref,) + refs[: count - 1]
    images = (img_ref,) + refs[count - 1 : 2 * count - 2]
    img_sum_ref, txt_sum_ref, loss_ref = refs[2 * count - 2 :]
    rows = txt_ref.shape[0]
    img_sum = txt_sum = loss = None
    for j in range(count):
        sign = eye_signs(rows) if j == 0 else -1.0
        arg = -sign * logits_of(par_ref, img_ref[...], texts[j][...])
        term = dot_n(weights(arg, sign), texts[j][...])
        img_sum = term if j == 0 else img_sum + term
        arg = -sign * logits_of(par_ref, txt_ref[...], images[j][...])
        term = dot_n(weights(arg, sign), images[j][...])
        txt_sum = term if j == 0 else txt_sum + term
        part = jnp.sum(softplus(arg), axis=0, keepdims=True)
        loss = part if j == 0 else loss + part
    img_sum_ref[...] = img_sum
    txt_sum_ref[...] = txt_sum
    loss_ref[...] = jnp.broadcast_to(jnp.sum(loss, axis=1, keepdims=True), loss_ref.shape)


def far_loss_kernel(n_img, pairs, par_ref, near_ref, *refs):
    images, texts, loss_ref = refs[:n_img], refs[n_img:-1], refs[-1]
    loss = None
    for image in images:
        for text in texts:
            part = jnp.sum(softplus(logits_of(par_ref, image[...], text[...])), axis=0, keepdims=True)
            loss = part if loss is None else loss + part
    total = near_ref[...] + jnp.broadcast_to(jnp.sum(loss, axis=1, keepdims=True), loss_ref.shape)
    loss_ref[...] = total / pairs


def sum_kernel(par_ref, own_ref, carry_ref, *refs):
    total = carry_ref[...]
    for block in refs[:-1]:
        arg = logits_of(par_ref, own_ref[...], block[...])
        total = total + dot_n(weights(arg, -1.0), block[...])
    refs[-1][...] = total


def far_sum(params, own, carry, blocks):
    rows, width = own.shape
    return kernel_call(
        sum_kernel,
        jax.ShapeDtypeStruct((rows, width), jnp.float32),
        (params, own, carry, *blocks),
        flops=4 * rows * rows * width * len(blocks),
    )


def last_kernel(count, par_ref, own_ref, carry_ref, unit_ref, inv_ref, *refs):
    blocks, (out_ref, buf, sems) = refs[:count], refs[count:]
    parts = sems.shape[0]
    step = buf.shape[0] // parts
    scale = par_ref[0:1, 0:1]
    gates = [weights(logits_of(par_ref, own_ref[...], block[...]), -1.0) for block in blocks]
    copies = []
    for k in range(parts):
        at = pl.ds(k * step, step)
        total = carry_ref[at, :]
        for gate, block in zip(gates, blocks):
            total = total + dot_n(gate[k * step : (k + 1) * step, :], block[...])
        grad = scale * total
        unit = unit_ref[at, :]
        inverse = inv_ref[at, 0:1]
        buf[at, :] = inverse * (grad - jnp.sum(grad * unit, axis=1, keepdims=True) * unit)
        copy = pltpu.make_async_copy(buf.at[at], out_ref.at[at], sems.at[k])
        copy.start()
        copies.append(copy)
    for copy in copies:
        copy.wait()


def finished(params, own, carry, unit, inverse, blocks):
    rows, width = own.shape
    return kernel_call(
        functools.partial(last_kernel, len(blocks)),
        jax.ShapeDtypeStruct((rows, width), jnp.float32),
        (params, own, carry, unit, inverse, *blocks),
        [pltpu.VMEM((rows, width), jnp.float32), pltpu.SemaphoreType.DMA((4,))],
        out_hbm=True,
        flops=4 * rows * rows * width * len(blocks),
    )


def summed(value):
    n_row, n_col = lax.axis_size("row"), lax.axis_size("col")
    if n_row & (n_row - 1) or n_col & (n_col - 1) or n_col < 2:
        return lax.psum(value, ("row", "col"))[0, :1]
    flips = [1]
    flips += [n_col << k | 1 for k in range(n_row.bit_length() - 1)]
    flips += [1 << k | 1 for k in range(1, n_col.bit_length() - 1)]
    for flip in flips:
        other = moved(value, ("row", "col"), lambda i: i ^ flip)
        value = value + other
    return value[0, :1]


def across(mine, cores):
    count = lax.axis_size("col")

    def target(i, hop):
        return (i // cores + hop) * cores % count + cores - 1 - i % cores

    return [moved(mine, "col", lambda i: target(i, hop)) for hop in range(1, count // cores)]


def partners(block, cores):
    return [moved(block, "col", lambda i: i // cores * cores + (i + core) % cores) for core in range(1, cores)]


def step(image_embed, text_embed, log_scale, bias):
    rows, width = image_embed.shape
    n_row = lax.axis_size("row")
    n_col = lax.axis_size("col")
    cores = 2 if n_col % 2 == 0 else 1
    params = jnp.broadcast_to(jnp.stack([jnp.exp(log_scale), bias]), (2, LANES))
    f32 = jnp.float32
    flops = 2 * rows * rows * width

    wide = jax.ShapeDtypeStruct((rows, width), f32)
    column = jax.ShapeDtypeStruct((rows, LANES), f32)
    txt_b = unit_parts(text_embed)[0].astype(jnp.bfloat16)
    txt_far = across(txt_b, cores)
    half = jax.ShapeDtypeStruct((rows, width), jnp.bfloat16)
    img_b, img_unit, img_inv = kernel_call(image_norm_kernel, (half, wide, column), (image_embed,))
    txt_unit, txt_inv = kernel_call(text_parts_kernel, (wide, column), (text_embed,))
    img_far = across(img_b, cores)
    txt_near = partners(txt_b, cores)
    img_near = partners(img_b, cores)
    terms = jax.ShapeDtypeStruct((1, LANES), f32)
    img_sum, txt_sum, loss = kernel_call(
        functools.partial(near_kernel, cores),
        (wide, wide, terms),
        (params, txt_b, img_b, *txt_near, *img_near),
        flops=4 * flops * cores,
    )
    if txt_far:
        txt_rest = [other for block in txt_far for other in partners(block, cores)]
        loss = kernel_call(
            functools.partial(far_loss_kernel, cores, rows * n_row * n_col),
            terms,
            (params, loss, img_b, *img_near, *txt_far),
            flops=flops * cores * len(txt_far),
        )
        img_rest = [other for block in img_far for other in partners(block, cores)]
        txt_sum = far_sum(params, txt_b, txt_sum, img_far)
    image_grad = finished(params, img_b, img_sum, img_unit, img_inv, txt_far + txt_rest)
    text_grad = finished(params, txt_b, txt_sum, txt_unit, txt_inv, img_rest)
    return (summed(loss), image_grad, text_grad)


def solution(mesh):
    in_specs = (P(("row", "col"), None), P(("row", "col"), None), P(), P())
    out_specs = (P(), P(("row", "col"), None), P(("row", "col"), None))
    return jax.shard_map(step, mesh=mesh, in_specs=in_specs, out_specs=out_specs, check_vma=False)
```

```python
import functools

import jax
import jax.numpy as jnp
from jax import lax
from jax.experimental import pallas as pl
from jax.experimental.pallas import tpu as pltpu
from jax.sharding import PartitionSpec as P


GRANT = 12 << 20
PARTS = 1
LANES = 128
VMEM = pl.BlockSpec(memory_space=pltpu.VMEM)
HBM = pl.BlockSpec(memory_space=pltpu.HBM)


def moved(value, axis, target):
    count = lax.psum(1, axis)
    return lax.ppermute(value, axis, [(i, target(i)) for i in range(count)])


def kernel_call(body, outs, ins, scratch=(), in_hbm=0, out_hbm=False, flops=0):
    return pl.pallas_call(
        body,
        out_shape=outs,
        in_specs=[HBM] * in_hbm + [VMEM] * (len(ins) - in_hbm),
        out_specs=jax.tree.map(lambda _: HBM if out_hbm else VMEM, outs),
        scratch_shapes=list(scratch),
        compiler_params=pltpu.CompilerParams(vmem_limit_bytes=GRANT),
        cost_estimate=pl.CostEstimate(flops=flops, bytes_accessed=0, transcendentals=0),
    )(*ins)


def dot_t(a, b):
    return lax.dot_general(a, b, (((1,), (1,)), ((), ())), preferred_element_type=jnp.float32)


def dot_n(a, b):
    return jnp.dot(a, b, preferred_element_type=jnp.float32)


def eye_signs(rows):
    eye = lax.broadcasted_iota(jnp.int32, (rows, rows), 0) == lax.broadcasted_iota(jnp.int32, (rows, rows), 1)
    return jnp.where(eye, 1.0, -1.0).astype(jnp.float32)


def softplus(v):
    return jnp.maximum(v, 0.0) + jnp.log1p(jnp.exp(-jnp.abs(v)))


def weights(arg, sign):
    return (-sign / (1.0 + jnp.exp(-arg))).astype(jnp.bfloat16)


def logits_of(par_ref, a, b):
    return par_ref[0:1, 0:1] * dot_t(a, b) + par_ref[1:2, 0:1]


def unit_parts(values):
    inverse = 1.0 / jnp.sqrt(jnp.sum(values * values, axis=1, keepdims=True) + 1e-06)
    return values * inverse, inverse


def norm_kernel(raw_ref, *refs):
    outs, (buf, sems) = refs[:-2], refs[-2:]
    parts = sems.shape[0]
    step = buf.shape[0] // parts
    spans = [pl.ds(k * step, step) for k in range(parts)]
    copies = [pltpu.make_async_copy(raw_ref.at[at], buf.at[at], sems.at[k]) for k, at in enumerate(spans)]
    for copy in copies:
        copy.start()
    for copy, at in zip(copies, spans):
        copy.wait()
        unit, inverse = unit_parts(buf[at, :])
        outs[0][at, :] = unit.astype(jnp.bfloat16)
        if len(outs) > 1:
            outs[1][at, :] = unit
            outs[2][at, :] = jnp.broadcast_to(inverse, (step, LANES))


def normed(raw, outs):
    rows, width = raw.shape
    return kernel_call(
        norm_kernel,
        outs,
        (pltpu.with_memory_space_constraint(raw, pltpu.HBM),),
        [pltpu.VMEM((rows, width), jnp.float32), pltpu.SemaphoreType.DMA((PARTS,))],
        in_hbm=1,
    )


def text_parts_kernel(raw_ref, unit_ref, inv_ref):
    unit, inverse = unit_parts(raw_ref[...])
    unit_ref[...] = unit
    inv_ref[...] = jnp.broadcast_to(inverse, inv_ref.shape)


def near_kernel(count, par_ref, txt_ref, img_ref, *refs):
    texts = (txt_ref,) + refs[: count - 1]
    images = (img_ref,) + refs[count - 1 : 2 * count - 2]
    img_sum_ref, txt_sum_ref, loss_ref = refs[2 * count - 2 :]
    rows = txt_ref.shape[0]
    img_sum = txt_sum = loss = None
    for j in range(count):
        sign = eye_signs(rows) if j == 0 else -1.0
        arg = -sign * logits_of(par_ref, img_ref[...], texts[j][...])
        term = dot_n(weights(arg, sign), texts[j][...])
        img_sum = term if j == 0 else img_sum + term
        arg = -sign * logits_of(par_ref, txt_ref[...], images[j][...])
        term = dot_n(weights(arg, sign), images[j][...])
        txt_sum = term if j == 0 else txt_sum + term
        part = jnp.sum(softplus(arg), axis=0, keepdims=True)
        loss = part if j == 0 else loss + part
    img_sum_ref[...] = img_sum
    txt_sum_ref[...] = txt_sum
    loss_ref[...] = jnp.broadcast_to(jnp.sum(loss, axis=1, keepdims=True), loss_ref.shape)


def far_loss_kernel(n_img, pairs, par_ref, near_ref, *refs):
    images, texts, loss_ref = refs[:n_img], refs[n_img:-1], refs[-1]
    loss = None
    for image in images:
        for text in texts:
            part = jnp.sum(softplus(logits_of(par_ref, image[...], text[...])), axis=0, keepdims=True)
            loss = part if loss is None else loss + part
    total = near_ref[...] + jnp.broadcast_to(jnp.sum(loss, axis=1, keepdims=True), loss_ref.shape)
    loss_ref[...] = total / pairs


def sum_kernel(par_ref, own_ref, carry_ref, *refs):
    total = carry_ref[...]
    for block in refs[:-1]:
        arg = logits_of(par_ref, own_ref[...], block[...])
        total = total + dot_n(weights(arg, -1.0), block[...])
    refs[-1][...] = total


def far_sum(params, own, carry, blocks):
    rows, width = own.shape
    return kernel_call(
        sum_kernel,
        jax.ShapeDtypeStruct((rows, width), jnp.float32),
        (params, own, carry, *blocks),
        flops=4 * rows * rows * width * len(blocks),
    )


def last_kernel(count, par_ref, own_ref, carry_ref, unit_ref, inv_ref, *refs):
    blocks, (out_ref, buf, sems) = refs[:count], refs[count:]
    parts = sems.shape[0]
    step = buf.shape[0] // parts
    scale = par_ref[0:1, 0:1]
    gates = [weights(logits_of(par_ref, own_ref[...], block[...]), -1.0) for block in blocks]
    copies = []
    for k in range(parts):
        at = pl.ds(k * step, step)
        total = carry_ref[at, :]
        for gate, block in zip(gates, blocks):
            total = total + dot_n(gate[k * step : (k + 1) * step, :], block[...])
        grad = scale * total
        unit = unit_ref[at, :]
        inverse = inv_ref[at, 0:1]
        buf[at, :] = inverse * (grad - jnp.sum(grad * unit, axis=1, keepdims=True) * unit)
        copy = pltpu.make_async_copy(buf.at[at], out_ref.at[at], sems.at[k])
        copy.start()
        copies.append(copy)
    for copy in copies:
        copy.wait()


def finished(params, own, carry, unit, inverse, blocks):
    rows, width = own.shape
    return kernel_call(
        functools.partial(last_kernel, len(blocks)),
        jax.ShapeDtypeStruct((rows, width), jnp.float32),
        (params, own, carry, unit, inverse, *blocks),
        [pltpu.VMEM((rows, width), jnp.float32), pltpu.SemaphoreType.DMA((4,))],
        out_hbm=True,
        flops=4 * rows * rows * width * len(blocks),
    )


def summed(value):
    n_row, n_col = lax.axis_size("row"), lax.axis_size("col")
    if n_row & (n_row - 1) or n_col & (n_col - 1) or n_col < 2:
        return lax.psum(value, ("row", "col"))[0, :1]
    flips = [1]
    flips += [n_col << k | 1 for k in reversed(range(n_row.bit_length() - 1))]
    flips += [1 << k | 1 for k in range(1, n_col.bit_length() - 1)]
    for flip in flips:
        other = moved(value, ("row", "col"), lambda i: i ^ flip)
        value = value + other
    return value[0, :1]


def across(mine, cores):
    count = lax.axis_size("col")

    def target(i, hop):
        return (i // cores + hop) * cores % count + cores - 1 - i % cores

    return [moved(mine, "col", lambda i: target(i, hop)) for hop in range(1, count // cores)]


def partners(block, cores):
    return [moved(block, "col", lambda i: i // cores * cores + (i + core) % cores) for core in range(1, cores)]


def step(image_embed, text_embed, log_scale, bias):
    rows, width = image_embed.shape
    n_row = lax.axis_size("row")
    n_col = lax.axis_size("col")
    cores = 2 if n_col % 2 == 0 else 1
    params = jnp.broadcast_to(jnp.stack([jnp.exp(log_scale), bias]), (2, LANES))
    f32 = jnp.float32
    flops = 2 * rows * rows * width

    wide = jax.ShapeDtypeStruct((rows, width), f32)
    column = jax.ShapeDtypeStruct((rows, LANES), f32)
    half = jax.ShapeDtypeStruct((rows, width), jnp.bfloat16)
    txt_b = normed(text_embed, half)
    txt_far = across(txt_b, cores)
    img_b, img_unit, img_inv = normed(image_embed, (half, wide, column))
    txt_unit, txt_inv = kernel_call(text_parts_kernel, (wide, column), (text_embed,))
    img_far = across(img_b, cores)
    txt_near = partners(txt_b, cores)
    img_near = partners(img_b, cores)
    terms = jax.ShapeDtypeStruct((1, LANES), f32)
    img_sum, txt_sum, loss = kernel_call(
        functools.partial(near_kernel, cores),
        (wide, wide, terms),
        (params, txt_b, img_b, *txt_near, *img_near),
        flops=4 * flops * cores,
    )
    if txt_far:
        txt_rest = [other for block in txt_far for other in partners(block, cores)]
        loss = kernel_call(
            functools.partial(far_loss_kernel, cores, rows * n_row * n_col),
            terms,
            (params, loss, img_b, *img_near, *txt_far),
            flops=flops * cores * len(txt_far),
        )
        img_rest = [other for block in img_far for other in partners(block, cores)]
        txt_sum = far_sum(params, txt_b, txt_sum, img_far)
    image_grad = finished(params, img_b, img_sum, img_unit, img_inv, txt_far + txt_rest)
    text_grad = finished(params, txt_b, txt_sum, txt_unit, txt_inv, img_rest)
    return (summed(loss), image_grad, text_grad)


def solution(mesh):
    in_specs = (P(("row", "col"), None), P(("row", "col"), None), P(), P())
    out_specs = (P(), P(("row", "col"), None), P(("row", "col"), None))
    return jax.shard_map(step, mesh=mesh, in_specs=in_specs, out_specs=out_specs, check_vma=False)
```

```python
import functools

import jax
import jax.numpy as jnp
from jax import lax
from jax.experimental import pallas as pl
from jax.experimental.pallas import tpu as pltpu
from jax.sharding import PartitionSpec as P


GRANT = 12 << 20
PARTS = 1
LANES = 128
VMEM = pl.BlockSpec(memory_space=pltpu.VMEM)
HBM = pl.BlockSpec(memory_space=pltpu.HBM)


def moved(value, axis, target):
    count = lax.psum(1, axis)
    return lax.ppermute(value, axis, [(i, target(i)) for i in range(count)])


def kernel_call(body, outs, ins, scratch=(), in_hbm=0, out_hbm=False, flops=0):
    return pl.pallas_call(
        body,
        out_shape=outs,
        in_specs=[HBM] * in_hbm + [VMEM] * (len(ins) - in_hbm),
        out_specs=jax.tree.map(lambda _: HBM if out_hbm else VMEM, outs),
        scratch_shapes=list(scratch),
        compiler_params=pltpu.CompilerParams(vmem_limit_bytes=GRANT),
        cost_estimate=pl.CostEstimate(flops=flops, bytes_accessed=0, transcendentals=0),
    )(*ins)


def dot_t(a, b):
    return lax.dot_general(a, b, (((1,), (1,)), ((), ())), preferred_element_type=jnp.float32)


def dot_n(a, b):
    return jnp.dot(a, b, preferred_element_type=jnp.float32)


def eye_signs(rows):
    eye = lax.broadcasted_iota(jnp.int32, (rows, rows), 0) == lax.broadcasted_iota(jnp.int32, (rows, rows), 1)
    return jnp.where(eye, 1.0, -1.0).astype(jnp.float32)


def softplus(v):
    return jnp.maximum(v, 0.0) + jnp.log1p(jnp.exp(-jnp.abs(v)))


def weights(arg, sign):
    return (-sign / (1.0 + jnp.exp(-arg))).astype(jnp.bfloat16)


def logits_of(par_ref, a, b):
    return par_ref[0:1, 0:1] * dot_t(a, b) + par_ref[1:2, 0:1]


def unit_parts(values):
    inverse = 1.0 / jnp.sqrt(jnp.sum(values * values, axis=1, keepdims=True) + 1e-06)
    return values * inverse, inverse


def norm_kernel(raw_ref, *refs):
    outs, (buf, sems) = refs[:-2], refs[-2:]
    parts = sems.shape[0]
    step = buf.shape[0] // parts
    spans = [pl.ds(k * step, step) for k in range(parts)]
    copies = [pltpu.make_async_copy(raw_ref.at[at], buf.at[at], sems.at[k]) for k, at in enumerate(spans)]
    for copy in copies:
        copy.start()
    for copy, at in zip(copies, spans):
        copy.wait()
        unit, inverse = unit_parts(buf[at, :])
        outs[0][at, :] = unit.astype(jnp.bfloat16)
        if len(outs) > 1:
            outs[1][at, :] = unit
            outs[2][at, :] = jnp.broadcast_to(inverse, (step, LANES))


def normed(raw, outs):
    rows, width = raw.shape
    return kernel_call(
        norm_kernel,
        outs,
        (pltpu.with_memory_space_constraint(raw, pltpu.HBM),),
        [pltpu.VMEM((rows, width), jnp.float32), pltpu.SemaphoreType.DMA((PARTS,))],
        in_hbm=1,
    )


def parts_kernel(raw_ref, unit_ref, inv_ref, buf, sem):
    copy = pltpu.make_async_copy(raw_ref, buf, sem)
    copy.start()
    copy.wait()
    unit, inverse = unit_parts(buf[...])
    unit_ref[...] = unit
    inv_ref[...] = jnp.broadcast_to(inverse, inv_ref.shape)


def copy_kernel(from_ref, to_ref):
    to_ref[...] = from_ref[...]


def near_kernel(count, par_ref, txt_ref, img_ref, *refs):
    texts = (txt_ref,) + refs[: count - 1]
    images = (img_ref,) + refs[count - 1 : 2 * count - 2]
    img_sum_ref, txt_sum_ref, pair_ref, loss_ref = refs[2 * count - 2 :]
    rows = txt_ref.shape[0]
    img_sum = txt_sum = loss = None
    for j in range(count):
        sign = eye_signs(rows) if j == 0 else -1.0
        pair_ref[pl.ds(j * rows, rows), :] = images[j][...]
        arg = -sign * logits_of(par_ref, img_ref[...], texts[j][...])
        term = dot_n(weights(arg, sign), texts[j][...])
        img_sum = term if j == 0 else img_sum + term
        arg = -sign * logits_of(par_ref, txt_ref[...], images[j][...])
        term = dot_n(weights(arg, sign), images[j][...])
        txt_sum = term if j == 0 else txt_sum + term
        part = jnp.sum(softplus(arg), axis=0, keepdims=True)
        loss = part if j == 0 else loss + part
    img_sum_ref[...] = img_sum
    txt_sum_ref[...] = txt_sum
    loss_ref[...] = loss


def far_loss_kernel(pairs, par_ref, near_ref, pair_ref, *refs):
    total = near_ref[...]
    for text in refs[:-1]:
        part = jnp.sum(softplus(logits_of(par_ref, text[...], pair_ref[...])), axis=0, keepdims=True)
        for j in range(part.shape[1] // LANES):
            total = total + part[:, j * LANES : (j + 1) * LANES]
    refs[-1][...] = jnp.broadcast_to(jnp.sum(total, axis=1, keepdims=True) / pairs, refs[-1].shape)


def sum_kernel(par_ref, own_ref, carry_ref, *refs):
    total = carry_ref[...]
    for block in refs[:-1]:
        arg = logits_of(par_ref, own_ref[...], block[...])
        total = total + dot_n(weights(arg, -1.0), block[...])
    refs[-1][...] = total


def far_sum(params, own, carry, blocks):
    rows, width = own.shape
    return kernel_call(
        sum_kernel,
        jax.ShapeDtypeStruct((rows, width), jnp.float32),
        (params, own, carry, *blocks),
        flops=4 * rows * rows * width * len(blocks),
    )


def last_kernel(count, par_ref, own_ref, carry_ref, unit_ref, inv_ref, *refs):
    blocks, (out_ref, buf, sems) = refs[:count], refs[count:]
    parts = sems.shape[0]
    step = buf.shape[0] // parts
    scale = par_ref[0:1, 0:1]
    gates = [weights(logits_of(par_ref, own_ref[...], block[...]), -1.0) for block in blocks]
    copies = []
    for k in range(parts):
        at = pl.ds(k * step, step)
        total = carry_ref[at, :]
        for gate, block in zip(gates, blocks):
            total = total + dot_n(gate[k * step : (k + 1) * step, :], block[...])
        grad = scale * total
        unit = unit_ref[at, :]
        inverse = inv_ref[at, 0:1]
        buf[at, :] = inverse * (grad - jnp.sum(grad * unit, axis=1, keepdims=True) * unit)
        copy = pltpu.make_async_copy(buf.at[at], out_ref.at[at], sems.at[k])
        copy.start()
        copies.append(copy)
    for copy in copies:
        copy.wait()


def finished(params, own, carry, unit, inverse, blocks):
    rows, width = own.shape
    return kernel_call(
        functools.partial(last_kernel, len(blocks)),
        jax.ShapeDtypeStruct((rows, width), jnp.float32),
        (params, own, carry, unit, inverse, *blocks),
        [pltpu.VMEM((rows, width), jnp.float32), pltpu.SemaphoreType.DMA((4,))],
        out_hbm=True,
        flops=4 * rows * rows * width * len(blocks),
    )


def summed(value):
    n_row, n_col = lax.axis_size("row"), lax.axis_size("col")
    if n_row & (n_row - 1) or n_col & (n_col - 1) or n_col < 2:
        return jnp.sum(lax.psum(value, ("row", "col")), axis=1)
    flips = [1]
    flips += [n_col << k | 1 for k in reversed(range(n_row.bit_length() - 1))]
    flips += [1 << k | 1 for k in range(1, n_col.bit_length() - 1)]
    for flip in flips:
        other = moved(value, ("row", "col"), lambda i: i ^ flip)
        value = value + other
    return value[0, :1]


def across(mine, cores):
    count = lax.axis_size("col")

    def target(i, hop):
        return (i // cores + hop) * cores % count + cores - 1 - i % cores

    return [moved(mine, "col", lambda i: target(i, hop)) for hop in range(1, count // cores)]


def partners(block, cores):
    return [moved(block, "col", lambda i: i // cores * cores + (i + core) % cores) for core in range(1, cores)]


def step(image_embed, text_embed, log_scale, bias):
    rows, width = image_embed.shape
    n_row = lax.axis_size("row")
    n_col = lax.axis_size("col")
    cores = 2 if n_col % 2 == 0 else 1
    params = jnp.broadcast_to(jnp.stack([jnp.exp(log_scale), bias]), (2, LANES))
    f32 = jnp.float32
    flops = 2 * rows * rows * width

    wide = jax.ShapeDtypeStruct((rows, width), f32)
    column = jax.ShapeDtypeStruct((rows, LANES), f32)
    half = jax.ShapeDtypeStruct((rows, width), jnp.bfloat16)
    txt_b = normed(text_embed, half)
    txt_far = across(txt_b, cores)
    img_b, img_unit, img_inv = normed(image_embed, (half, wide, column))
    txt_unit, txt_inv = kernel_call(
        parts_kernel,
        (wide, column),
        (pltpu.with_memory_space_constraint(text_embed, pltpu.HBM),),
        [pltpu.VMEM((rows, width), f32), pltpu.SemaphoreType.DMA],
        in_hbm=1,
    )
    img_far = across(img_b, cores)
    txt_near = partners(txt_b, cores)
    img_near = partners(img_b, cores)
    terms = jax.ShapeDtypeStruct((1, LANES), f32)
    pair = jax.ShapeDtypeStruct((cores * rows, width), jnp.bfloat16)
    img_sum, txt_sum, pair, loss = kernel_call(
        functools.partial(near_kernel, cores),
        (wide, wide, pair, terms),
        (params, txt_b, img_b, *txt_near, *img_near),
        flops=4 * flops * cores,
    )
    params = kernel_call(copy_kernel, jax.ShapeDtypeStruct(params.shape, f32), (params,))
    if txt_far:
        txt_rest = [other for block in txt_far for other in partners(block, cores)]
        loss = kernel_call(
            functools.partial(far_loss_kernel, rows * n_row * n_col),
            terms,
            (params, loss, pair, *txt_far),
            flops=flops * cores * len(txt_far),
        )
        img_rest = [other for block in img_far for other in partners(block, cores)]
        txt_sum = far_sum(params, txt_b, txt_sum, img_far)
    image_grad = finished(params, img_b, img_sum, img_unit, img_inv, txt_far + txt_rest)
    text_grad = finished(params, txt_b, txt_sum, txt_unit, txt_inv, img_rest)
    return (summed(loss), image_grad, text_grad)


def solution(mesh):
    in_specs = (P(("row", "col"), None), P(("row", "col"), None), P(), P())
    out_specs = (P(), P(("row", "col"), None), P(("row", "col"), None))
    return jax.shard_map(step, mesh=mesh, in_specs=in_specs, out_specs=out_specs, check_vma=False)
```

```python
import functools

import jax
import jax.numpy as jnp
from jax import lax
from jax.experimental import pallas as pl
from jax.experimental.pallas import tpu as pltpu
from jax.sharding import PartitionSpec as P


GRANT = 12 << 20
PARTS = 1
LANES = 128
VMEM = pl.BlockSpec(memory_space=pltpu.VMEM)
HBM = pl.BlockSpec(memory_space=pltpu.HBM)


def moved(value, axis, target):
    count = lax.psum(1, axis)
    return lax.ppermute(value, axis, [(i, target(i)) for i in range(count)])


def kernel_call(body, outs, ins, scratch=(), in_hbm=0, out_hbm=False, flops=0):
    return pl.pallas_call(
        body,
        out_shape=outs,
        in_specs=[HBM] * in_hbm + [VMEM] * (len(ins) - in_hbm),
        out_specs=jax.tree.map(lambda _: HBM if out_hbm else VMEM, outs),
        scratch_shapes=list(scratch),
        compiler_params=pltpu.CompilerParams(vmem_limit_bytes=GRANT),
        cost_estimate=pl.CostEstimate(flops=flops, bytes_accessed=0, transcendentals=0),
    )(*ins)


def dot_t(a, b):
    return lax.dot_general(a, b, (((1,), (1,)), ((), ())), preferred_element_type=jnp.float32)


def dot_n(a, b):
    return jnp.dot(a, b, preferred_element_type=jnp.float32)


def eye_signs(rows):
    eye = lax.broadcasted_iota(jnp.int32, (rows, rows), 0) == lax.broadcasted_iota(jnp.int32, (rows, rows), 1)
    return jnp.where(eye, 1.0, -1.0).astype(jnp.float32)


def softplus(v):
    return jnp.maximum(v, 0.0) + jnp.log1p(jnp.exp(-jnp.abs(v)))


def weights(arg, sign):
    return (-sign / (1.0 + jnp.exp(-arg))).astype(jnp.bfloat16)


def logits_of(par_ref, a, b):
    return par_ref[0:1, 0:1] * dot_t(a, b) + par_ref[1:2, 0:1]


def unit_parts(values):
    inverse = 1.0 / jnp.sqrt(jnp.sum(values * values, axis=1, keepdims=True) + 1e-06)
    return values * inverse, inverse


def norm_kernel(raw_ref, *refs):
    outs, (buf, sems) = refs[:-2], refs[-2:]
    parts = sems.shape[0]
    step = buf.shape[0] // parts
    spans = [pl.ds(k * step, step) for k in range(parts)]
    copies = [pltpu.make_async_copy(raw_ref.at[at], buf.at[at], sems.at[k]) for k, at in enumerate(spans)]
    for copy in copies:
        copy.start()
    for copy, at in zip(copies, spans):
        copy.wait()
        unit, inverse = unit_parts(buf[at, :])
        outs[0][at, :] = unit.astype(jnp.bfloat16)
        if len(outs) > 1:
            outs[1][at, :] = unit
            outs[2][at, :] = jnp.broadcast_to(inverse, (step, LANES))


def normed(raw, outs):
    rows, width = raw.shape
    return kernel_call(
        norm_kernel,
        outs,
        (pltpu.with_memory_space_constraint(raw, pltpu.HBM),),
        [pltpu.VMEM((rows, width), jnp.float32), pltpu.SemaphoreType.DMA((PARTS,))],
        in_hbm=1,
    )


def parts_kernel(raw_ref, unit_ref, inv_ref, buf, sem):
    copy = pltpu.make_async_copy(raw_ref, buf, sem)
    copy.start()
    copy.wait()
    unit, inverse = unit_parts(buf[...])
    unit_ref[...] = unit
    inv_ref[...] = jnp.broadcast_to(inverse, inv_ref.shape)


def copy_kernel(from_ref, to_ref):
    to_ref[...] = from_ref[...]


def near_kernel(count, par_ref, txt_ref, img_ref, *refs):
    texts = (txt_ref,) + refs[: count - 1]
    images = (img_ref,) + refs[count - 1 : 2 * count - 2]
    img_sum_ref, txt_sum_ref, pair_ref, loss_ref = refs[2 * count - 2 :]
    rows = txt_ref.shape[0]
    img_sum = txt_sum = loss = None
    for j in range(count):
        sign = eye_signs(rows) if j == 0 else -1.0
        pair_ref[pl.ds(j * rows, rows), :] = images[j][...]
        arg = -sign * logits_of(par_ref, img_ref[...], texts[j][...])
        term = dot_n(weights(arg, sign), texts[j][...])
        img_sum = term if j == 0 else img_sum + term
        arg = -sign * logits_of(par_ref, txt_ref[...], images[j][...])
        term = dot_n(weights(arg, sign), images[j][...])
        txt_sum = term if j == 0 else txt_sum + term
        part = jnp.sum(softplus(arg), axis=0, keepdims=True)
        loss = part if j == 0 else loss + part
    img_sum_ref[...] = img_sum
    txt_sum_ref[...] = txt_sum
    loss_ref[...] = loss


def far_loss_kernel(pairs, par_ref, near_ref, pair_ref, *refs):
    total = near_ref[...]
    for text in refs[:-1]:
        part = jnp.sum(softplus(logits_of(par_ref, text[...], pair_ref[...])), axis=0, keepdims=True)
        for j in range(part.shape[1] // LANES):
            total = total + part[:, j * LANES : (j + 1) * LANES]
    refs[-1][...] = jnp.broadcast_to(jnp.sum(total, axis=1, keepdims=True) / pairs, refs[-1].shape)


def sum_kernel(par_ref, own_ref, carry_ref, *refs):
    total = carry_ref[...]
    for block in refs[:-1]:
        arg = logits_of(par_ref, own_ref[...], block[...])
        total = total + dot_n(weights(arg, -1.0), block[...])
    refs[-1][...] = total


def far_sum(params, own, carry, blocks):
    rows, width = own.shape
    return kernel_call(
        sum_kernel,
        jax.ShapeDtypeStruct((rows, width), jnp.float32),
        (params, own, carry, *blocks),
        flops=4 * rows * rows * width * len(blocks),
    )


def last_kernel(count, par_ref, own_ref, carry_ref, unit_ref, inv_ref, *refs):
    blocks, (out_ref, buf, sems) = refs[:count], refs[count:]
    parts = sems.shape[0]
    step = buf.shape[0] // parts
    scale = par_ref[0:1, 0:1]
    gates = [weights(logits_of(par_ref, own_ref[...], block[...]), -1.0) for block in blocks]
    copies = []
    for k in range(parts):
        at = pl.ds(k * step, step)
        total = carry_ref[at, :]
        for gate, block in zip(gates, blocks):
            total = total + dot_n(gate[k * step : (k + 1) * step, :], block[...])
        grad = scale * total
        unit = unit_ref[at, :]
        inverse = inv_ref[at, 0:1]
        buf[at, :] = inverse * (grad - jnp.sum(grad * unit, axis=1, keepdims=True) * unit)
        copy = pltpu.make_async_copy(buf.at[at], out_ref.at[at], sems.at[k])
        copy.start()
        copies.append(copy)
    for copy in copies:
        copy.wait()


def finished(params, own, carry, unit, inverse, blocks):
    rows, width = own.shape
    return kernel_call(
        functools.partial(last_kernel, len(blocks)),
        jax.ShapeDtypeStruct((rows, width), jnp.float32),
        (params, own, carry, unit, inverse, *blocks),
        [pltpu.VMEM((rows, width), jnp.float32), pltpu.SemaphoreType.DMA((2,))],
        out_hbm=True,
        flops=4 * rows * rows * width * len(blocks),
    )


def summed(value):
    n_row, n_col = lax.axis_size("row"), lax.axis_size("col")
    if n_row & (n_row - 1) or n_col & (n_col - 1) or n_col < 2:
        return jnp.sum(lax.psum(value, ("row", "col")), axis=1)
    flips = [1]
    top = n_row.bit_length() - 2
    flips += [n_col << k | 1 for k in (top, *range(top)) if k >= 0]
    flips += [1 << k | 1 for k in range(1, n_col.bit_length() - 1)]
    for flip in flips:
        other = moved(value, ("row", "col"), lambda i: i ^ flip)
        value = value + other
    return value[0, :1]


def across(mine, cores):
    count = lax.axis_size("col")

    def target(i, hop):
        return (i // cores + hop) * cores % count + cores - 1 - i % cores

    return [moved(mine, "col", lambda i: target(i, hop)) for hop in range(1, count // cores)]


def partners(block, cores):
    return [moved(block, "col", lambda i: i // cores * cores + (i + core) % cores) for core in range(1, cores)]


def step(image_embed, text_embed, log_scale, bias):
    rows, width = image_embed.shape
    n_row = lax.axis_size("row")
    n_col = lax.axis_size("col")
    cores = 2 if n_col % 2 == 0 else 1
    params = jnp.broadcast_to(jnp.stack([jnp.exp(log_scale), bias]), (2, LANES))
    f32 = jnp.float32
    flops = 2 * rows * rows * width

    wide = jax.ShapeDtypeStruct((rows, width), f32)
    column = jax.ShapeDtypeStruct((rows, LANES), f32)
    half = jax.ShapeDtypeStruct((rows, width), jnp.bfloat16)
    txt_b = normed(text_embed, half)
    txt_far = across(txt_b, cores)
    img_b, img_unit, img_inv = normed(image_embed, (half, wide, column))
    txt_unit, txt_inv = kernel_call(
        parts_kernel,
        (wide, column),
        (pltpu.with_memory_space_constraint(text_embed, pltpu.HBM),),
        [pltpu.VMEM((rows, width), f32), pltpu.SemaphoreType.DMA],
        in_hbm=1,
    )
    img_far = across(img_b, cores)
    txt_near = partners(txt_b, cores)
    img_near = partners(img_b, cores)
    terms = jax.ShapeDtypeStruct((1, LANES), f32)
    pair = jax.ShapeDtypeStruct((cores * rows, width), jnp.bfloat16)
    img_sum, txt_sum, pair, loss = kernel_call(
        functools.partial(near_kernel, cores),
        (wide, wide, pair, terms),
        (params, txt_b, img_b, *txt_near, *img_near),
        flops=4 * flops * cores,
    )
    params = kernel_call(copy_kernel, jax.ShapeDtypeStruct(params.shape, f32), (params,))
    if txt_far:
        txt_rest = [other for block in txt_far for other in partners(block, cores)]
        loss = kernel_call(
            functools.partial(far_loss_kernel, rows * n_row * n_col),
            terms,
            (params, loss, pair, *txt_far),
            flops=flops * cores * len(txt_far),
        )
        img_rest = [other for block in img_far for other in partners(block, cores)]
        txt_sum = far_sum(params, txt_b, txt_sum, img_far)
    image_grad = finished(params, img_b, img_sum, img_unit, img_inv, txt_far + txt_rest)
    text_grad = finished(params, txt_b, txt_sum, txt_unit, txt_inv, img_rest)
    return (summed(loss), image_grad, text_grad)


def solution(mesh):
    in_specs = (P(("row", "col"), None), P(("row", "col"), None), P(), P())
    out_specs = (P(), P(("row", "col"), None), P(("row", "col"), None))
    return jax.shard_map(step, mesh=mesh, in_specs=in_specs, out_specs=out_specs, check_vma=False)
```

```python
import functools

import jax
import jax.numpy as jnp
from jax import lax
from jax.experimental import pallas as pl
from jax.experimental.pallas import tpu as pltpu
from jax.sharding import PartitionSpec as P


GRANT = 12 << 20
PARTS = 1
LANES = 128
VMEM = pl.BlockSpec(memory_space=pltpu.VMEM)
HBM = pl.BlockSpec(memory_space=pltpu.HBM)


def moved(value, axis, target):
    count = lax.psum(1, axis)
    return lax.ppermute(value, axis, [(i, target(i)) for i in range(count)])


def kernel_call(body, outs, ins, scratch=(), in_hbm=0, out_hbm=False, flops=0):
    return pl.pallas_call(
        body,
        out_shape=outs,
        in_specs=[HBM] * in_hbm + [VMEM] * (len(ins) - in_hbm),
        out_specs=jax.tree.map(lambda _: HBM if out_hbm else VMEM, outs),
        scratch_shapes=list(scratch),
        compiler_params=pltpu.CompilerParams(vmem_limit_bytes=GRANT),
        cost_estimate=pl.CostEstimate(flops=flops, bytes_accessed=0, transcendentals=0),
    )(*ins)


def dot_t(a, b):
    return lax.dot_general(a, b, (((1,), (1,)), ((), ())), preferred_element_type=jnp.float32)


def dot_n(a, b):
    return jnp.dot(a, b, preferred_element_type=jnp.float32)


def eye_signs(rows):
    eye = lax.broadcasted_iota(jnp.int32, (rows, rows), 0) == lax.broadcasted_iota(jnp.int32, (rows, rows), 1)
    return jnp.where(eye, 1.0, -1.0).astype(jnp.float32)


def softplus(v):
    return jnp.maximum(v, 0.0) + jnp.log1p(jnp.exp(-jnp.abs(v)))


def weights(arg, sign):
    return (-sign / (1.0 + jnp.exp(-arg))).astype(jnp.bfloat16)


def logits_of(par_ref, a, b):
    return par_ref[0:1, 0:1] * dot_t(a, b) + par_ref[1:2, 0:1]


def unit_parts(values):
    inverse = 1.0 / jnp.sqrt(jnp.sum(values * values, axis=1, keepdims=True) + 1e-06)
    return values * inverse, inverse


def norm_kernel(raw_ref, *refs):
    outs, (buf, sems) = refs[:-2], refs[-2:]
    parts = sems.shape[0]
    step = buf.shape[0] // parts
    spans = [pl.ds(k * step, step) for k in range(parts)]
    copies = [pltpu.make_async_copy(raw_ref.at[at], buf.at[at], sems.at[k]) for k, at in enumerate(spans)]
    for copy in copies:
        copy.start()
    for copy, at in zip(copies, spans):
        copy.wait()
        unit, inverse = unit_parts(buf[at, :])
        outs[0][at, :] = unit.astype(jnp.bfloat16)
        if len(outs) > 1:
            outs[1][at, :] = unit
            outs[2][at, :] = jnp.broadcast_to(inverse, (step, LANES))


def normed(raw, outs):
    rows, width = raw.shape
    return kernel_call(
        norm_kernel,
        outs,
        (pltpu.with_memory_space_constraint(raw, pltpu.HBM),),
        [pltpu.VMEM((rows, width), jnp.float32), pltpu.SemaphoreType.DMA((PARTS,))],
        in_hbm=1,
    )


def parts_kernel(raw_ref, unit_ref, inv_ref, buf, sem):
    copy = pltpu.make_async_copy(raw_ref, buf, sem)
    copy.start()
    copy.wait()
    unit, inverse = unit_parts(buf[...])
    unit_ref[...] = unit
    inv_ref[...] = jnp.broadcast_to(inverse, inv_ref.shape)


def copy_kernel(from_ref, to_ref):
    to_ref[...] = from_ref[...]


def near_kernel(count, par_ref, txt_ref, img_ref, *refs):
    texts = (txt_ref,) + refs[: count - 1]
    images = (img_ref,) + refs[count - 1 : 2 * count - 2]
    img_sum_ref, txt_sum_ref, pair_ref, loss_ref = refs[2 * count - 2 :]
    rows = txt_ref.shape[0]
    img_sum = txt_sum = loss = None
    for j in range(count):
        sign = eye_signs(rows) if j == 0 else -1.0
        pair_ref[pl.ds(j * rows, rows), :] = images[j][...]
        arg = -sign * logits_of(par_ref, img_ref[...], texts[j][...])
        term = dot_n(weights(arg, sign), texts[j][...])
        img_sum = term if j == 0 else img_sum + term
        arg = -sign * logits_of(par_ref, txt_ref[...], images[j][...])
        term = dot_n(weights(arg, sign), images[j][...])
        txt_sum = term if j == 0 else txt_sum + term
        part = jnp.sum(softplus(arg), axis=0, keepdims=True)
        loss = part if j == 0 else loss + part
    img_sum_ref[...] = img_sum
    txt_sum_ref[...] = txt_sum
    loss_ref[...] = loss


def far_loss_kernel(pairs, par_ref, near_ref, pair_ref, *refs):
    total = near_ref[...]
    for text in refs[:-1]:
        part = jnp.sum(softplus(logits_of(par_ref, text[...], pair_ref[...])), axis=0, keepdims=True)
        for j in range(part.shape[1] // LANES):
            total = total + part[:, j * LANES : (j + 1) * LANES]
    refs[-1][...] = jnp.broadcast_to(jnp.sum(total, axis=1, keepdims=True) / pairs, refs[-1].shape)


def sum_kernel(par_ref, own_ref, carry_ref, *refs):
    total = carry_ref[...]
    for block in refs[:-1]:
        arg = logits_of(par_ref, own_ref[...], block[...])
        total = total + dot_n(weights(arg, -1.0), block[...])
    refs[-1][...] = total


def far_sum(params, own, carry, blocks):
    rows, width = own.shape
    return kernel_call(
        sum_kernel,
        jax.ShapeDtypeStruct((rows, width), jnp.float32),
        (params, own, carry, *blocks),
        flops=4 * rows * rows * width * len(blocks),
    )


def last_kernel(count, par_ref, own_ref, carry_ref, unit_ref, inv_ref, *refs):
    blocks, (out_ref, buf, sems) = refs[:count], refs[count:]
    parts = sems.shape[0]
    step = buf.shape[0] // parts
    scale = par_ref[0:1, 0:1]
    gates = [weights(logits_of(par_ref, own_ref[...], block[...]), -1.0) for block in blocks]
    copies = []
    for k in range(parts):
        at = pl.ds(k * step, step)
        total = carry_ref[at, :]
        for gate, block in zip(gates, blocks):
            total = total + dot_n(gate[k * step : (k + 1) * step, :], block[...])
        grad = scale * total
        unit = unit_ref[at, :]
        inverse = inv_ref[at, 0:1]
        buf[at, :] = inverse * (grad - jnp.sum(grad * unit, axis=1, keepdims=True) * unit)
        copy = pltpu.make_async_copy(buf.at[at], out_ref.at[at], sems.at[k])
        copy.start()
        copies.append(copy)
    for copy in copies:
        copy.wait()


def finished(params, own, carry, unit, inverse, blocks):
    rows, width = own.shape
    return kernel_call(
        functools.partial(last_kernel, len(blocks)),
        jax.ShapeDtypeStruct((rows, width), jnp.float32),
        (params, own, carry, unit, inverse, *blocks),
        [pltpu.VMEM((rows, width), jnp.float32), pltpu.SemaphoreType.DMA((2,))],
        out_hbm=True,
        flops=4 * rows * rows * width * len(blocks),
    )


def summed(value):
    n_row, n_col = lax.axis_size("row"), lax.axis_size("col")
    if n_row & (n_row - 1) or n_col & (n_col - 1) or n_col < 2:
        return jnp.sum(lax.psum(value, ("row", "col")), axis=1)
    top = n_row.bit_length() - 2
    rows = [n_col << k | 1 for k in (top, *reversed(range(top))) if k >= 0]
    flips = [1, *rows[:1], *(1 << k | 1 for k in range(1, n_col.bit_length() - 1)), *rows[1:]]
    for flip in flips:
        other = moved(value, ("row", "col"), lambda i: i ^ flip)
        value = value + other
    return value[0, :1]


def across(mine, cores):
    count = lax.axis_size("col")

    def target(i, hop):
        return (i // cores + hop) * cores % count + cores - 1 - i % cores

    return [moved(mine, "col", lambda i: target(i, hop)) for hop in range(1, count // cores)]


def partners(block, cores):
    return [moved(block, "col", lambda i: i // cores * cores + (i + core) % cores) for core in range(1, cores)]


def step(image_embed, text_embed, log_scale, bias):
    rows, width = image_embed.shape
    n_row = lax.axis_size("row")
    n_col = lax.axis_size("col")
    cores = 2 if n_col % 2 == 0 else 1
    params = jnp.broadcast_to(jnp.stack([jnp.exp(log_scale), bias]), (2, LANES))
    f32 = jnp.float32
    flops = 2 * rows * rows * width

    wide = jax.ShapeDtypeStruct((rows, width), f32)
    column = jax.ShapeDtypeStruct((rows, LANES), f32)
    half = jax.ShapeDtypeStruct((rows, width), jnp.bfloat16)
    txt_b = normed(text_embed, half)
    txt_far = across(txt_b, cores)
    img_b, img_unit, img_inv = normed(image_embed, (half, wide, column))
    txt_unit, txt_inv = kernel_call(
        parts_kernel,
        (wide, column),
        (pltpu.with_memory_space_constraint(text_embed, pltpu.HBM),),
        [pltpu.VMEM((rows, width), f32), pltpu.SemaphoreType.DMA],
        in_hbm=1,
    )
    img_far = across(img_b, cores)
    txt_near = partners(txt_b, cores)
    img_near = partners(img_b, cores)
    terms = jax.ShapeDtypeStruct((1, LANES), f32)
    pair = jax.ShapeDtypeStruct((cores * rows, width), jnp.bfloat16)
    img_sum, txt_sum, pair, loss = kernel_call(
        functools.partial(near_kernel, cores),
        (wide, wide, pair, terms),
        (params, txt_b, img_b, *txt_near, *img_near),
        flops=4 * flops * cores,
    )
    params = kernel_call(copy_kernel, jax.ShapeDtypeStruct(params.shape, f32), (params,))
    if txt_far:
        txt_rest = [other for block in txt_far for other in partners(block, cores)]
        loss = kernel_call(
            functools.partial(far_loss_kernel, rows * n_row * n_col),
            terms,
            (params, loss, pair, *txt_far),
            flops=flops * cores * len(txt_far),
        )
        img_rest = [other for block in img_far for other in partners(block, cores)]
        txt_sum = far_sum(params, txt_b, txt_sum, img_far)
    image_grad = finished(params, img_b, img_sum, img_unit, img_inv, txt_far + txt_rest)
    text_grad = finished(params, txt_b, txt_sum, txt_unit, txt_inv, img_rest)
    return (summed(loss), image_grad, text_grad)


def solution(mesh):
    in_specs = (P(("row", "col"), None), P(("row", "col"), None), P(), P())
    out_specs = (P(), P(("row", "col"), None), P(("row", "col"), None))
    return jax.shard_map(step, mesh=mesh, in_specs=in_specs, out_specs=out_specs, check_vma=False)
```
